32 devices in a mesh: row: 8 (over z, core), col: 4 (over y, x).
Axes of the slice: x: 2, y: 2, z: 4, core: 2. Of those that a mesh axis runs over, the one named last changes fastest.
Arguments:
- reflectivity: float32 [32, 256, 1024], P(('row', 'col')), may hold values from 0 to 40
- scan_hour: int32 [32], replicated, may hold values from 0 to 3, as said below
- basin_ids: int32 [256, 8], P('row', 'col'), may hold values from 0 to 255, as said below
Outputs:
- hourly_depth: float32 [4, 256, 1024], P(None, 'row', 'col')
- basin_depth: float32 [256, 4], P(('row', 'col'))
The draws below stay inside these ranges and needn't reach their ends.
Inputs may be any that keep to these rules, and one draw needn't show every extreme that they name: scan_hour starts at 0, never falls, rises by at most one from one scan to the next, and every hour has 1 to 12 scans. `basin_ids`: every basin is named by at least one segment, and all segments of a basin lie in one aligned block of 8 grid rows.
All inputs are finite; a program needn't handle non-finite values.
Results may differ from the reference program's by a relative error of at most 0.00021.
Values sent between devices are 32-bit elements; how exact they have to be, the bound alone decides.
A program may use at most 64 MiB of HBM per device.

```python
import math
import jax
import jax.numpy as jnp
from jax import lax

SEG = 128
BASIN_ROWS = 8
SCANS = 32
HOURS = 4
NY = 256
NX = 1024
BASINS = 256


def draw_scan_hour(key, part):
    spare = 11
    extra = SCANS - HOURS
    slots = jax.random.permutation(jax.random.fold_in(key, 5), HOURS * spare).astype(jnp.int32)
    chosen = slots[:extra] // spare
    hour_range = jnp.arange(HOURS, dtype=jnp.int32)
    counts = 1 + jnp.sum((chosen[:, None] == hour_range[None, :]).astype(jnp.int32), axis=0)
    ends = jnp.cumsum(counts).astype(jnp.int32)
    positions = jnp.arange(SCANS, dtype=jnp.int32)
    hours = jnp.sum((ends[None, :HOURS - 1] <= positions[:, None]).astype(jnp.int32), axis=1)
    return hours.astype(jnp.int32)


def block_order(block_key):
    return jax.random.permutation(block_key, BASIN_ROWS * (NX // SEG)).astype(jnp.int32)


def draw_basin_ids(key, part):
    seg_count = NX // SEG
    block_count = NY // BASIN_ROWS
    block_cells = BASIN_ROWS * seg_count
    block_keys = jax.random.split(jax.random.fold_in(key, 3), block_count)
    ranks = jax.vmap(block_order)(block_keys).astype(jnp.int32)
    spread = jax.random.randint(jax.random.fold_in(key, 4), (block_count, block_cells), 0, seg_count).astype(jnp.int32)
    local = jnp.where(ranks < seg_count, ranks, spread).astype(jnp.int32)
    base = jnp.arange(block_count, dtype=jnp.int32)[:, None] * seg_count + local
    labels = jax.random.permutation(jax.random.fold_in(key, 7), BASINS).astype(jnp.int32)
    return labels[base].reshape(NY, seg_count).astype(jnp.int32)


def shard_levels(own_key, dims, cuts, least, top_value):
    def one(axis_at, blocks):
        heights = jax.random.uniform(jax.random.fold_in(jax.random.fold_in(own_key, 6), axis_at), (blocks,), jnp.float32, least / len(cuts), top_value / len(cuts))
        return jnp.repeat(jnp.exp(heights), dims[axis_at] // blocks).reshape((-1,) + (1,) * (len(dims) - axis_at - 1))

    loudness = one(*cuts[0])
    for cut in cuts[1:]:
        loudness = loudness * one(*cut)
    return loudness


def setup_inputs(seed: int = 0) -> dict:
    key_list = jax.random.split(jax.random.key(seed), 4)
    return {
        "reflectivity": jnp.clip(40.0 * jax.random.uniform(key_list[0], (SCANS, NY, NX), jnp.float32) ** shard_levels(key_list[0], (SCANS, NY, NX), ((0, 32),), -0.2, 0.2), 0.0, 40.0),
        "scan_hour": draw_scan_hour(jax.random.fold_in(key_list[3], 71), 0),
        "basin_ids": draw_basin_ids(jax.random.fold_in(key_list[3], 71), 0),
    }


slope_db = math.log(10.0) / 16.0
offset_zr = math.log(200.0) / 1.6


def rain_depth(reflect):
    return jnp.exp(reflect * slope_db - offset_zr) / 12.0


def reference(reflectivity, scan_hour, basin_ids):
    def accumulate(running, scan_item):
        radar_frame, hour_slot = scan_item
        return running.at[hour_slot].add(rain_depth(radar_frame)), None

    initial = jnp.zeros((HOURS, NY, NX), jnp.float32)
    hourly, unused = lax.scan(accumulate, initial, (reflectivity, scan_hour))
    segment = hourly.reshape(HOURS, NY, NX // SEG, SEG).sum(axis=3).reshape(HOURS, -1)
    flat_ids = basin_ids.reshape(-1).astype(jnp.int32)
    totals = jax.ops.segment_sum(segment.T, flat_ids, num_segments=BASINS)
    pixels = jax.ops.segment_sum(jnp.full(flat_ids.shape, float(SEG), jnp.float32), flat_ids, num_segments=BASINS)
    return hourly, totals / pixels[:, None]
```

```python
import functools
import math

import jax
import jax.numpy as jnp
from jax import lax
from jax.experimental import pallas as pl
from jax.experimental.pallas import tpu as pltpu
from jax.sharding import PartitionSpec as P

SEG = 128
BASIN_ROWS = 8
HOUR_SCANS = 12
CORES = 2
MESH = pl.DeviceIdType.MESH

slope_db = math.log(10.0) / 16.0
offset_zr = math.log(200.0) / 1.6 + math.log(12.0)


def kernel(
    dims,
    refl_ref,
    hour_ref,
    ids_ref,
    hourly_ref,
    basin_ref,
    frame,
    hours,
    ids,
    gather,
    part,
    zrecv,
    psend,
    precv,
    local_sem,
    own_sem,
    in_send,
    in_recv,
    z_send,
    z_recv,
    b_send,
    b_recv,
):
    row_devices, col_devices, hour_count, slots, tile_rows, tile_cols, owned = dims
    planes = row_devices // CORES
    members = CORES * col_devices
    devices = row_devices * col_devices
    scan_block = gather.shape[2]
    scan_count = hour_ref.shape[0]
    plane_scans = members * scan_block
    segs = tile_cols // SEG

    row = lax.axis_index("row")
    col = lax.axis_index("col")
    plane = row // CORES
    core = row % CORES
    mine = core * col_devices + col
    me = row * col_devices + col

    def first_hour(p):
        return (p * plane_scans) // HOUR_SCANS

    def hour_span(p):
        tail = scan_count - plane_scans - p * plane_scans
        return hour_count - tail // HOUR_SCANS - first_hour(p)

    def member_at(k):
        other = (mine + k) % members
        return other, plane * CORES + other // col_devices, other % col_devices

    load_frame = pltpu.make_async_copy(refl_ref, frame, local_sem.at[0])
    load_hours = pltpu.make_async_copy(hour_ref, hours, local_sem.at[1])
    load_ids = pltpu.make_async_copy(ids_ref, ids, local_sem.at[2])
    load_frame.start()
    load_hours.start()
    load_ids.start()

    def block_of(source, d, c, q):
        rows = pl.ds(pl.multiple_of((d * CORES + c) * tile_rows, 8), tile_rows)
        cols = pl.ds(pl.multiple_of(q * tile_cols, 128), tile_cols)
        return source.at[:, rows, cols]

    barrier = pltpu.get_barrier_semaphore()
    for k in range(1, members):
        _, r, q = member_at(k)
        pl.semaphore_signal(barrier, inc=1, device_id=(r, q), device_id_type=MESH)
    for k in range(1, planes):
        r = ((plane + k) % planes) * CORES + core
        pl.semaphore_signal(barrier, inc=1, device_id=(r, col), device_id_type=MESH)

    own_copies = []
    for d in range(planes):
        own = pltpu.make_async_copy(
            block_of(refl_ref, d, core, col), gather.at[d, mine], own_sem.at[d]
        )
        own.start()
        own_copies.append(own)

    low = plane < planes // 2
    order = []
    for t in range(planes - 1):
        down = planes - 1 - t
        down = jnp.where(down > plane, down, down - 1)
        up = jnp.where(t < plane, t, t + 1)
        order.append(jnp.where(low, down, up))
    order.append(plane)

    pl.semaphore_wait(barrier, members - 1 + planes - 1)
    load_frame.wait()

    def in_copy(d, k):
        other, r, q = member_at(k)
        return pltpu.make_async_remote_copy(
            src_ref=block_of(frame, d, other // col_devices, q),
            dst_ref=gather.at[d, mine],
            send_sem=in_send.at[d, other],
            recv_sem=in_recv.at[d, mine],
            device_id=(r, q),
            device_id_type=MESH,
        )

    def in_arrival(d, k):
        other, r, q = member_at(k)
        return pltpu.make_async_remote_copy(
            src_ref=gather.at[d, other],
            dst_ref=gather.at[d, other],
            send_sem=in_send.at[d, other],
            recv_sem=in_recv.at[d, other],
            device_id=(r, q),
            device_id_type=MESH,
        )

    for d in order:
        for k in range(1, members):
            in_copy(d, k).start()

    load_hours.wait()
    load_ids.wait()
    for own in own_copies:
        own.wait()

    lane = lax.broadcasted_iota(jnp.int32, (tile_rows, 128), 1)
    owner_rows = lax.broadcasted_iota(jnp.int32, (devices, tile_rows), 0)
    owner_hot = []
    lane_hot = []
    for g in range(segs):
        id_row = ids[g : g + 1, :]
        owner = lax.div(id_row, jnp.full_like(id_row, owned))
        owner_hot.append((owner_rows == owner).astype(jnp.float32))
        within = (id_row - owner * owned).astype(jnp.float32)
        spread = jnp.transpose(jnp.broadcast_to(within, (128, tile_rows)))
        lane_hot.append(((lane % owned) == spread.astype(jnp.int32)).astype(jnp.float32))
    owner_all = jnp.concatenate(owner_hot, axis=1)

    base_hour = first_hour(plane)
    span = hour_span(plane)

    def z_copy(d, k):
        return pltpu.make_async_remote_copy(
            src_ref=part.at[d, k],
            dst_ref=zrecv.at[plane, k],
            send_sem=z_send.at[d, k],
            recv_sem=z_recv.at[plane, k],
            device_id=(d * CORES + core, col),
            device_id_type=MESH,
        )

    for t, d in enumerate(order):
        for k in range(1, members):
            in_arrival(d, k).wait_recv()
        sums = [jnp.zeros((tile_rows, tile_cols), jnp.float32)] * slots
        for i in range(members):
            for b in range(scan_block):
                hour = hours[plane * plane_scans + i * scan_block + b] - base_hour
                depth = jnp.exp(gather[d, i, b] * slope_db - offset_zr)
                for k in range(slots):
                    sums[k] = sums[k] + jnp.where(hour == k, depth, 0.0)
        if t < planes - 1:
            for k in range(slots):
                part[d, k] = sums[k]
            for k in range(slots):

                @pl.when(k < span)
                def _():
                    z_copy(d, k).start()
        else:
            for k in range(slots):
                zrecv[plane, k] = sums[k]

    for p in range(planes):

        @pl.when(p != plane)
        def _():
            for k in range(hour_span(p)):
                pltpu.make_async_remote_copy(
                    src_ref=zrecv.at[p, k],
                    dst_ref=zrecv.at[p, k],
                    send_sem=z_send.at[p, k],
                    recv_sem=z_recv.at[p, k],
                    device_id=(p * CORES + core, col),
                    device_id_type=MESH,
                ).wait_recv()

    lanes = [jnp.zeros((tile_rows, 128), jnp.float32) for _ in range(segs)]
    for h in range(hour_count):
        total = None
        for p in range(planes):
            if first_hour(p) <= h < first_hour(p) + hour_span(p):
                term = zrecv[p, h - first_hour(p)]
                total = term if total is None else total + term
        hourly_ref[h] = total
        for g in range(segs):
            value = jnp.sum(total[:, g * SEG : (g + 1) * SEG], axis=1, keepdims=True)
            lanes[g] = jnp.where(lane // owned == h, value, lanes[g])
    stacked = []
    for g in range(segs):
        filled = jnp.where(lane // owned == hour_count, float(SEG), lanes[g])
        stacked.append(filled * lane_hot[g])
    partial = lax.dot_general(
        owner_all,
        jnp.concatenate(stacked, axis=0),
        (((1,), (0,)), ((), ())),
        precision=lax.Precision.HIGHEST,
        preferred_element_type=jnp.float32,
    )
    for o in range(devices):
        psend[o] = partial[o : o + 1, :]

    def b_copy(k):
        other = (me + k) % devices
        return pltpu.make_async_remote_copy(
            src_ref=psend.at[other],
            dst_ref=precv.at[me],
            send_sem=b_send.at[other],
            recv_sem=b_recv.at[me],
            device_id=(other // col_devices, other % col_devices),
            device_id_type=MESH,
        )

    def b_start(k, carry):
        b_copy(k).start()
        return carry

    lax.fori_loop(1, devices, b_start, 0)
    precv[me] = psend[me]

    for d in order:
        for k in range(1, members):
            in_copy(d, k).wait_send()
    for d in order[:-1]:
        for k in range(slots):

            @pl.when(k < span)
            def _():
                z_copy(d, k).wait_send()

    def b_wait(k, carry):
        other = (me + k) % devices
        arrival = pltpu.make_async_remote_copy(
            src_ref=psend.at[other],
            dst_ref=precv.at[other],
            send_sem=b_send.at[other],
            recv_sem=b_recv.at[other],
            device_id=(other // col_devices, other % col_devices),
            device_id_type=MESH,
        )
        arrival.wait_recv()
        arrival.wait_send()
        return carry

    lax.fori_loop(1, devices, b_wait, 0)
    total = jnp.sum(precv[...], axis=0)
    count = total[:, hour_count * owned : (hour_count + 1) * owned]
    for h in range(hour_count):
        basin_ref[h : h + 1, :] = total[:, h * owned : (h + 1) * owned] / count


def body(reflectivity, scan_hour, basin_ids):
    row_devices = lax.axis_size("row")
    col_devices = lax.axis_size("col")
    scan_block, grid_height, grid_width = reflectivity.shape
    tile_rows = grid_height // row_devices
    tile_cols = grid_width // col_devices
    scan_count = scan_hour.shape[0]
    hour_count = (scan_count + 10) // HOUR_SCANS + 1
    devices = row_devices * col_devices
    owned = grid_height * grid_width // (SEG * BASIN_ROWS) // devices
    planes = row_devices // CORES
    members = CORES * col_devices
    plane_scans = members * scan_block
    slots = max(
        hour_count
        - (scan_count - plane_scans * (p + 1)) // HOUR_SCANS
        - (p * plane_scans) // HOUR_SCANS
        for p in range(planes)
    )
    dims = (row_devices, col_devices, hour_count, slots, tile_rows, tile_cols, owned)
    dma = pltpu.SemaphoreType.DMA
    f32 = jnp.float32
    anywhere = pl.BlockSpec(memory_space=pl.ANY)
    inside = pl.BlockSpec(memory_space=pltpu.VMEM)
    hourly, basin = pl.pallas_call(
        functools.partial(kernel, dims),
        out_shape=(
            jax.ShapeDtypeStruct((hour_count, tile_rows, tile_cols), f32),
            jax.ShapeDtypeStruct((hour_count, owned), f32),
        ),
        in_specs=[anywhere] * 3,
        out_specs=(inside, inside),
        scratch_shapes=[
            pltpu.VMEM(reflectivity.shape, f32),
            pltpu.SMEM(scan_hour.shape, jnp.int32),
            pltpu.VMEM(basin_ids.shape[::-1], jnp.int32),
            pltpu.VMEM((planes, members, scan_block, tile_rows, tile_cols), f32),
            pltpu.VMEM((planes, slots, tile_rows, tile_cols), f32),
            pltpu.VMEM((planes, slots, tile_rows, tile_cols), f32),
            pltpu.VMEM((devices, 1, 128), f32),
            pltpu.VMEM((devices, 1, 128), f32),
            dma((3,)),
            dma((planes,)),
            dma((planes, members)),
            dma((planes, members)),
            dma((planes, slots)),
            dma((planes, slots)),
            dma((devices,)),
            dma((devices,)),
        ],
        compiler_params=pltpu.CompilerParams(collective_id=0, has_side_effects=True),
    )(reflectivity, scan_hour, basin_ids.T)
    return hourly, basin.T


def solution(mesh):
    placed = (P(("row", "col"), None, None), P(), P("row", "col"))
    return jax.shard_map(
        body,
        mesh=mesh,
        in_specs=placed,
        out_specs=(P(None, "row", "col"), P(("row", "col"), None)),
        check_vma=False,
    )
```

```python
import functools
import math

import jax
import jax.numpy as jnp
from jax import lax
from jax.experimental import pallas as pl
from jax.experimental.pallas import tpu as pltpu
from jax.sharding import PartitionSpec as P

SEG = 128
BASIN_ROWS = 8
HOUR_SCANS = 12
CORES = 2
MESH = pl.DeviceIdType.MESH

slope_db = math.log(10.0) / 16.0
offset_zr = math.log(200.0) / 1.6 + math.log(12.0)


def kernel(
    dims,
    refl_ref,
    hour_ref,
    ids_ref,
    hourly_ref,
    basin_ref,
    frame,
    hours,
    ids,
    gather,
    part,
    zrecv,
    plane_ids,
    all_ids,
    psend,
    precv,
    relay_sem,
    local_sem,
    own_sem,
    in_send,
    in_recv,
    z_send,
    z_recv,
    id_send,
    id_recv,
    idz_send,
    idz_recv,
    b_send,
    b_recv,
):
    row_devices, col_devices, hour_count, slots, tile_rows, tile_cols, owned = dims
    planes = row_devices // CORES
    members = CORES * col_devices
    devices = row_devices * col_devices
    scan_block = gather.shape[2]
    scan_count = hour_ref.shape[0]
    plane_scans = members * scan_block
    segs = tile_cols // SEG

    row = lax.axis_index("row")
    col = lax.axis_index("col")
    plane = row // CORES
    core = row % CORES
    mine = core * col_devices + col
    me = row * col_devices + col

    def first_hour(p):
        return (p * plane_scans) // HOUR_SCANS

    def hour_span(p):
        tail = scan_count - plane_scans - p * plane_scans
        return hour_count - tail // HOUR_SCANS - first_hour(p)

    def member_at(k):
        other = (mine + k) % members
        return other, plane * CORES + other // col_devices, other % col_devices

    load_frame = pltpu.make_async_copy(refl_ref, frame, local_sem.at[0])
    load_hours = pltpu.make_async_copy(hour_ref, hours, local_sem.at[1])
    load_ids = pltpu.make_async_copy(ids_ref, ids, local_sem.at[2])
    load_frame.start()
    load_hours.start()
    load_ids.start()
    load_own_ids = pltpu.make_async_copy(
        ids_ref, plane_ids.at[core * col_devices + col], local_sem.at[3]
    )
    load_own_ids.start()

    def block_of(source, d, c, q):
        rows = pl.ds(pl.multiple_of((d * CORES + c) * tile_rows, 8), tile_rows)
        cols = pl.ds(pl.multiple_of(q * tile_cols, 128), tile_cols)
        return source.at[:, rows, cols]

    barrier = pltpu.get_barrier_semaphore()
    for k in range(1, members):
        _, r, q = member_at(k)
        pl.semaphore_signal(barrier, inc=1, device_id=(r, q), device_id_type=MESH)
    def along_z(step):
        return ((plane + step) * CORES + core, col)

    @pl.when(plane > 0)
    def _():
        pl.semaphore_signal(barrier, inc=1, device_id=along_z(-1), device_id_type=MESH)

    @pl.when(plane < planes - 1)
    def _():
        pl.semaphore_signal(barrier, inc=1, device_id=along_z(1), device_id_type=MESH)

    own_copies = []
    for d in range(planes):
        own = pltpu.make_async_copy(
            block_of(refl_ref, d, core, col), gather.at[d, mine], own_sem.at[d]
        )
        own.start()
        own_copies.append(own)

    low = plane < planes // 2
    order = []
    for t in range(planes - 1):
        down = planes - 1 - t
        down = jnp.where(down > plane, down, down - 1)
        up = jnp.where(t < plane, t, t + 1)
        order.append(jnp.where(low, down, up))
    order.append(plane)

    load_ids.wait()
    load_frame.wait()
    beside = jnp.where(plane > 0, 1, 0) + jnp.where(plane < planes - 1, 1, 0)
    pl.semaphore_wait(barrier, members - 1 + beside)

    def id_copy(k):
        other, r, q = member_at(k)
        return pltpu.make_async_remote_copy(
            src_ref=ids,
            dst_ref=plane_ids.at[mine],
            send_sem=id_send.at[other],
            recv_sem=id_recv.at[mine],
            device_id=(r, q),
            device_id_type=MESH,
        )

    for k in range(1, members):
        id_copy(k).start()

    def in_copy(d, k):
        other, r, q = member_at(k)
        return pltpu.make_async_remote_copy(
            src_ref=block_of(frame, d, other // col_devices, q),
            dst_ref=gather.at[d, mine],
            send_sem=in_send.at[d, other],
            recv_sem=in_recv.at[d, mine],
            device_id=(r, q),
            device_id_type=MESH,
        )

    def in_arrival(d, k):
        other, r, q = member_at(k)
        return pltpu.make_async_remote_copy(
            src_ref=gather.at[d, other],
            dst_ref=gather.at[d, other],
            send_sem=in_send.at[d, other],
            recv_sem=in_recv.at[d, other],
            device_id=(r, q),
            device_id_type=MESH,
        )

    def send_chunk(d):
        for k in range(1, members):
            in_copy(d, k).start()

    early = max(1, planes - 2)
    for d in order[:early]:
        send_chunk(d)

    for j in range(planes - 2):

        @pl.when(plane > 0)
        def _():
            pl.semaphore_signal(
                relay_sem.at[1, j], inc=1, device_id=along_z(-1), device_id_type=MESH
            )

        @pl.when(plane < planes - 1)
        def _():
            pl.semaphore_signal(
                relay_sem.at[0, j], inc=1, device_id=along_z(1), device_id_type=MESH
            )

        @pl.when(plane > 0)
        def _():
            pl.semaphore_wait(relay_sem.at[0, j], 1)

        @pl.when(plane < planes - 1)
        def _():
            pl.semaphore_wait(relay_sem.at[1, j], 1)

    for k in range(1, members):
        other, r, q = member_at(k)
        pltpu.make_async_remote_copy(
            src_ref=ids,
            dst_ref=plane_ids.at[other],
            send_sem=id_send.at[other],
            recv_sem=id_recv.at[other],
            device_id=(r, q),
            device_id_type=MESH,
        ).wait_recv()
    load_own_ids.wait()

    def idz_copy(k, arrival=False):
        other = (plane + k) % planes
        return pltpu.make_async_remote_copy(
            src_ref=plane_ids,
            dst_ref=all_ids.at[other if arrival else plane],
            send_sem=idz_send.at[other],
            recv_sem=idz_recv.at[other if arrival else plane],
            device_id=(other * CORES + core, col),
            device_id_type=MESH,
        )

    for k in range(1, planes):
        idz_copy(k).start()
    all_ids[plane] = plane_ids[...]
    load_hours.wait()
    for own in own_copies:
        own.wait()

    base_hour = first_hour(plane)
    span = hour_span(plane)

    def z_copy(d, k):
        return pltpu.make_async_remote_copy(
            src_ref=part.at[d, k],
            dst_ref=zrecv.at[plane, k],
            send_sem=z_send.at[d, k],
            recv_sem=z_recv.at[plane, k],
            device_id=(d * CORES + core, col),
            device_id_type=MESH,
        )

    def b_copy(k):
        other = (me + k) % devices
        return pltpu.make_async_remote_copy(
            src_ref=psend,
            dst_ref=precv.at[me],
            send_sem=b_send.at[other],
            recv_sem=b_recv.at[me],
            device_id=(other // col_devices, other % col_devices),
            device_id_type=MESH,
        )

    basins = psend.shape[1]

    def sum_basins():
        lane = lax.broadcasted_iota(jnp.int32, (tile_rows, basins), 1)

        def row_block(r, carry):
            count, *totals = carry
            p = r // CORES
            c = r % CORES
            depths = []
            for b in range(scan_block):
                rows = pl.ds(pl.multiple_of(r * tile_rows, 8), tile_rows)
                depths.append(jnp.exp(frame[b, rows, :] * slope_db - offset_zr))
            tiles = [all_ids[p, c * col_devices + q] for q in range(col_devices)]
            columns = jnp.transpose(jnp.concatenate(tiles, axis=0).astype(jnp.float32))
            columns = columns.astype(jnp.int32)
            for g in range(segs * col_devices):
                hit = columns[:, g : g + 1] == lane
                count = count + jnp.where(hit, float(SEG), 0.0)
                for b in range(scan_block):
                    part_depth = depths[b][:, g * SEG : (g + 1) * SEG]
                    value = jnp.sum(part_depth, axis=1, keepdims=True)
                    totals[b] = totals[b] + jnp.where(hit, value, 0.0)
            return (count, *totals)

        zero = jnp.zeros((tile_rows, basins), jnp.float32)
        count, *totals = lax.fori_loop(0, row_devices, row_block, (zero,) * (scan_block + 1))
        for b in range(scan_block):
            psend[b : b + 1, :] = jnp.sum(totals[b], axis=0, keepdims=True)
        return jnp.sum(count, axis=0, keepdims=True)

    count = None
    for t, d in enumerate(order):
        if t == min(1, planes - 1):
            for k in range(1, planes):
                idz_copy(k, arrival=True).wait_recv()
            count = sum_basins()

            def b_start(k, carry):
                b_copy(k).start()
                return carry

            lax.fori_loop(1, devices, b_start, 0)
            precv[me] = psend[...]
            for late in order[early + 1 :]:
                send_chunk(late)
        for k in range(1, members):
            in_arrival(d, k).wait_recv()
        sums = [jnp.zeros((tile_rows, tile_cols), jnp.float32)] * slots
        for i in range(members):
            for b in range(scan_block):
                hour = hours[plane * plane_scans + i * scan_block + b] - base_hour
                depth = jnp.exp(gather[d, i, b] * slope_db - offset_zr)
                for k in range(slots):
                    sums[k] = sums[k] + jnp.where(hour == k, depth, 0.0)
        if t < planes - 1:
            for k in range(slots):
                part[d, k] = sums[k]
            for k in range(slots):

                @pl.when(k < span)
                def _():
                    z_copy(d, k).start()

            if t == 0:
                send_chunk(order[early])
        else:
            for k in range(slots):
                zrecv[plane, k] = sums[k]

    for p in range(planes):

        @pl.when(p != plane)
        def _():
            for k in range(hour_span(p)):
                pltpu.make_async_remote_copy(
                    src_ref=zrecv.at[p, k],
                    dst_ref=zrecv.at[p, k],
                    send_sem=z_send.at[p, k],
                    recv_sem=z_recv.at[p, k],
                    device_id=(p * CORES + core, col),
                    device_id_type=MESH,
                ).wait_recv()

    for h in range(hour_count):
        total = None
        for p in range(planes):
            if first_hour(p) <= h < first_hour(p) + hour_span(p):
                term = zrecv[p, h - first_hour(p)]
                total = term if total is None else total + term
        hourly_ref[h] = total

    for k in range(1, members):
        id_copy(k).wait_send()
    for k in range(1, planes):
        idz_copy(k).wait_send()
    for d in order:
        for k in range(1, members):
            in_copy(d, k).wait_send()
    for d in order[:-1]:
        for k in range(slots):

            @pl.when(k < span)
            def _():
                z_copy(d, k).wait_send()

    def b_wait(k, carry):
        other = (me + k) % devices
        arrival = pltpu.make_async_remote_copy(
            src_ref=psend,
            dst_ref=precv.at[other],
            send_sem=b_send.at[other],
            recv_sem=b_recv.at[other],
            device_id=(other // col_devices, other % col_devices),
            device_id_type=MESH,
        )
        arrival.wait_recv()
        arrival.wait_send()
        return carry

    lax.fori_loop(1, devices, b_wait, 0)
    hour_rows = lax.broadcasted_iota(jnp.int32, (hour_count, basins), 0)
    total = jnp.zeros((hour_count, basins), jnp.float32)
    for o in range(devices):
        for b in range(scan_block):
            hour = hours[o * scan_block + b]
            total = total + jnp.where(hour_rows == hour, precv[o, b : b + 1, :], 0.0)
    mean = total / count
    mean = pltpu.roll(mean, (basins - me * owned) % basins, 1)
    basin_ref[...] = mean[:, :owned]


def body(reflectivity, scan_hour, basin_ids):
    row_devices = lax.axis_size("row")
    col_devices = lax.axis_size("col")
    scan_block, grid_height, grid_width = reflectivity.shape
    tile_rows = grid_height // row_devices
    tile_cols = grid_width // col_devices
    scan_count = scan_hour.shape[0]
    hour_count = (scan_count + 10) // HOUR_SCANS + 1
    devices = row_devices * col_devices
    owned = grid_height * grid_width // (SEG * BASIN_ROWS) // devices
    planes = row_devices // CORES
    members = CORES * col_devices
    plane_scans = members * scan_block
    slots = max(
        hour_count
        - (scan_count - plane_scans * (p + 1)) // HOUR_SCANS
        - (p * plane_scans) // HOUR_SCANS
        for p in range(planes)
    )
    dims = (row_devices, col_devices, hour_count, slots, tile_rows, tile_cols, owned)
    dma = pltpu.SemaphoreType.DMA
    f32 = jnp.float32
    anywhere = pl.BlockSpec(memory_space=pltpu.HBM)
    inside = pl.BlockSpec(memory_space=pltpu.VMEM)
    hourly, basin = pl.pallas_call(
        functools.partial(kernel, dims),
        out_shape=(
            jax.ShapeDtypeStruct((hour_count, tile_rows, tile_cols), f32),
            jax.ShapeDtypeStruct((hour_count, owned), f32),
        ),
        in_specs=[anywhere] * 3,
        out_specs=(inside, inside),
        scratch_shapes=[
            pltpu.VMEM(reflectivity.shape, f32),
            pltpu.SMEM(scan_hour.shape, jnp.int32),
            pltpu.VMEM(basin_ids.shape[::-1], jnp.int32),
            pltpu.VMEM((planes, members, scan_block, tile_rows, tile_cols), f32),
            pltpu.VMEM((planes, slots, tile_rows, tile_cols), f32),
            pltpu.VMEM((planes, slots, tile_rows, tile_cols), f32),
            pltpu.VMEM((members,) + basin_ids.shape[::-1], jnp.int32),
            pltpu.VMEM((planes, members) + basin_ids.shape[::-1], jnp.int32),
            pltpu.VMEM((scan_block, devices * owned), f32),
            pltpu.VMEM((devices, scan_block, devices * owned), f32),
            pltpu.SemaphoreType.REGULAR((2, max(1, planes - 2))),
            dma((4,)),
            dma((planes,)),
            dma((planes, members)),
            dma((planes, members)),
            dma((planes, slots)),
            dma((planes, slots)),
            dma((members,)),
            dma((members,)),
            dma((planes,)),
            dma((planes,)),
            dma((devices,)),
            dma((devices,)),
        ],
        compiler_params=pltpu.CompilerParams(
            collective_id=0, has_side_effects=True, vmem_limit_bytes=40 * 2**20
        ),
    )(reflectivity, scan_hour, basin_ids.T)
    return hourly, basin.T


def solution(mesh):
    placed = (P(("row", "col"), None, None), P(), P("row", "col"))
    return jax.shard_map(
        body,
        mesh=mesh,
        in_specs=placed,
        out_specs=(P(None, "row", "col"), P(("row", "col"), None)),
        check_vma=False,
    )
```

```python
import functools
import math

import jax
import jax.numpy as jnp
from jax import lax
from jax.experimental import pallas as pl
from jax.experimental.pallas import tpu as pltpu
from jax.sharding import PartitionSpec as P

SEG = 128
BASIN_ROWS = 8
HOUR_SCANS = 12
CORES = 2
MESH = pl.DeviceIdType.MESH

slope_db = math.log(10.0) / 16.0
offset_zr = math.log(200.0) / 1.6 + math.log(12.0)


def kernel(
    dims,
    refl_ref,
    hour_ref,
    ids_ref,
    hourly_ref,
    basin_ref,
    frame,
    hours,
    ids,
    gather,
    part,
    zrecv,
    plane_ids,
    all_ids,
    psend,
    precv,
    relay_sem,
    local_sem,
    own_sem,
    in_send,
    in_recv,
    z_send,
    z_recv,
    id_send,
    id_recv,
    idz_send,
    idz_recv,
    b_send,
    b_recv,
):
    row_devices, col_devices, hour_count, slots, tile_rows, tile_cols, owned = dims
    planes = row_devices // CORES
    members = CORES * col_devices
    devices = row_devices * col_devices
    scan_block = gather.shape[2]
    scan_count = hour_ref.shape[0]
    plane_scans = members * scan_block
    segs = tile_cols // SEG

    row = lax.axis_index("row")
    col = lax.axis_index("col")
    plane = row // CORES
    core = row % CORES
    mine = core * col_devices + col
    me = row * col_devices + col

    def first_hour(p):
        return (p * plane_scans) // HOUR_SCANS

    def hour_span(p):
        tail = scan_count - plane_scans - p * plane_scans
        return hour_count - tail // HOUR_SCANS - first_hour(p)

    def member_at(k):
        dc = k // col_devices
        dq = k % col_devices
        half = col_devices // 2
        qq = ((col // 2 + dq // 2) % half) * 2 + (col + dq) % 2
        other = ((core + dc) % CORES) * col_devices + qq
        return other, plane * CORES + other // col_devices, other % col_devices

    load_frame = pltpu.make_async_copy(refl_ref, frame, local_sem.at[0])
    load_hours = pltpu.make_async_copy(hour_ref, hours, local_sem.at[1])
    load_ids = pltpu.make_async_copy(ids_ref, ids, local_sem.at[2])
    load_frame.start()
    load_hours.start()
    load_ids.start()
    load_own_ids = pltpu.make_async_copy(
        ids_ref, plane_ids.at[core * col_devices + col], local_sem.at[3]
    )
    load_own_ids.start()

    def block_of(source, d, c, q):
        rows = pl.ds(pl.multiple_of((d * CORES + c) * tile_rows, 8), tile_rows)
        cols = pl.ds(pl.multiple_of(q * tile_cols, 128), tile_cols)
        return source.at[:, rows, cols]

    barrier = pltpu.get_barrier_semaphore()
    for k in range(1, members):
        _, r, q = member_at(k)
        pl.semaphore_signal(barrier, inc=1, device_id=(r, q), device_id_type=MESH)
    def along_z(step):
        return ((plane + step) * CORES + core, col)

    @pl.when(plane > 0)
    def _():
        pl.semaphore_signal(barrier, inc=1, device_id=along_z(-1), device_id_type=MESH)

    @pl.when(plane < planes - 1)
    def _():
        pl.semaphore_signal(barrier, inc=1, device_id=along_z(1), device_id_type=MESH)

    own_copies = []
    for d in range(planes):
        own = pltpu.make_async_copy(
            block_of(refl_ref, d, core, col), gather.at[d, mine], own_sem.at[d]
        )
        own.start()
        own_copies.append(own)

    low = plane < planes // 2
    order = []
    for t in range(planes - 1):
        down = planes - 1 - t
        down = jnp.where(down > plane, down, down - 1)
        up = jnp.where(t < plane, t, t + 1)
        order.append(jnp.where(low, down, up))
    order.append(plane)

    load_ids.wait()
    load_frame.wait()
    beside = jnp.where(plane > 0, 1, 0) + jnp.where(plane < planes - 1, 1, 0)
    pl.semaphore_wait(barrier, members - 1 + beside)

    def id_copy(k):
        other, r, q = member_at(k)
        return pltpu.make_async_remote_copy(
            src_ref=ids,
            dst_ref=plane_ids.at[mine],
            send_sem=id_send.at[other],
            recv_sem=id_recv.at[mine],
            device_id=(r, q),
            device_id_type=MESH,
        )

    for k in range(1, members):
        id_copy(k).start()

    def in_copy(d, k):
        other, r, q = member_at(k)
        return pltpu.make_async_remote_copy(
            src_ref=block_of(frame, d, other // col_devices, q),
            dst_ref=gather.at[d, mine],
            send_sem=in_send.at[d, other],
            recv_sem=in_recv.at[d, mine],
            device_id=(r, q),
            device_id_type=MESH,
        )

    def in_arrival(d, k):
        other, r, q = member_at(k)
        return pltpu.make_async_remote_copy(
            src_ref=gather.at[d, other],
            dst_ref=gather.at[d, other],
            send_sem=in_send.at[d, other],
            recv_sem=in_recv.at[d, other],
            device_id=(r, q),
            device_id_type=MESH,
        )

    def send_chunk(d):
        for k in range(1, members):
            in_copy(d, k).start()

    early = max(1, planes - 1)
    for d in order[:early]:
        send_chunk(d)

    for j in range(planes - 2):

        @pl.when(plane > 0)
        def _():
            pl.semaphore_signal(
                relay_sem.at[1, j], inc=1, device_id=along_z(-1), device_id_type=MESH
            )

        @pl.when(plane < planes - 1)
        def _():
            pl.semaphore_signal(
                relay_sem.at[0, j], inc=1, device_id=along_z(1), device_id_type=MESH
            )

        @pl.when(plane > 0)
        def _():
            pl.semaphore_wait(relay_sem.at[0, j], 1)

        @pl.when(plane < planes - 1)
        def _():
            pl.semaphore_wait(relay_sem.at[1, j], 1)

    for k in range(1, members):
        other, r, q = member_at(k)
        pltpu.make_async_remote_copy(
            src_ref=ids,
            dst_ref=plane_ids.at[other],
            send_sem=id_send.at[other],
            recv_sem=id_recv.at[other],
            device_id=(r, q),
            device_id_type=MESH,
        ).wait_recv()
    load_own_ids.wait()

    def idz_copy(k, arrival=False):
        other = (plane + k) % planes
        return pltpu.make_async_remote_copy(
            src_ref=plane_ids,
            dst_ref=all_ids.at[other if arrival else plane],
            send_sem=idz_send.at[other],
            recv_sem=idz_recv.at[other if arrival else plane],
            device_id=(other * CORES + core, col),
            device_id_type=MESH,
        )

    for k in range(1, planes):
        idz_copy(k).start()
    all_ids[plane] = plane_ids[...]
    load_hours.wait()
    for own in own_copies:
        own.wait()

    base_hour = first_hour(plane)
    span = hour_span(plane)

    def z_copy(d, k):
        return pltpu.make_async_remote_copy(
            src_ref=part.at[d, k],
            dst_ref=zrecv.at[plane, k],
            send_sem=z_send.at[d, k],
            recv_sem=z_recv.at[plane, k],
            device_id=(d * CORES + core, col),
            device_id_type=MESH,
        )

    def b_copy(k):
        other = (me + k) % devices
        return pltpu.make_async_remote_copy(
            src_ref=psend,
            dst_ref=precv.at[me],
            send_sem=b_send.at[other],
            recv_sem=b_recv.at[me],
            device_id=(other // col_devices, other % col_devices),
            device_id_type=MESH,
        )

    basins = psend.shape[1]

    def sum_basins():
        lane = lax.broadcasted_iota(jnp.int32, (tile_rows, basins), 1)

        def row_block(r, carry):
            count, *totals = carry
            p = r // CORES
            c = r % CORES
            depths = []
            for b in range(scan_block):
                rows = pl.ds(pl.multiple_of(r * tile_rows, 8), tile_rows)
                depths.append(jnp.exp(frame[b, rows, :] * slope_db - offset_zr))
            tiles = [all_ids[p, c * col_devices + q] for q in range(col_devices)]
            columns = jnp.transpose(jnp.concatenate(tiles, axis=0).astype(jnp.float32))
            columns = columns.astype(jnp.int32)
            for g in range(segs * col_devices):
                hit = columns[:, g : g + 1] == lane
                count = count + jnp.where(hit, float(SEG), 0.0)
                for b in range(scan_block):
                    part_depth = depths[b][:, g * SEG : (g + 1) * SEG]
                    value = jnp.sum(part_depth, axis=1, keepdims=True)
                    totals[b] = totals[b] + jnp.where(hit, value, 0.0)
            return (count, *totals)

        zero = jnp.zeros((tile_rows, basins), jnp.float32)
        count, *totals = lax.fori_loop(
            0, row_devices, row_block, (zero,) * (scan_block + 1), unroll=4
        )
        for b in range(scan_block):
            psend[b : b + 1, :] = jnp.sum(totals[b], axis=0, keepdims=True)
        return jnp.sum(count, axis=0, keepdims=True)

    count = None
    for t, d in enumerate(order):
        if t == min(1, planes - 1):
            for k in range(1, planes):
                idz_copy(k, arrival=True).wait_recv()
            count = sum_basins()

            def b_start(k, carry):
                b_copy(k).start()
                return carry

            lax.fori_loop(1, devices, b_start, 0, unroll=True)
            precv[me] = psend[...]
            for late in order[early:]:
                send_chunk(late)
        for k in range(1, members):
            in_arrival(d, k).wait_recv()
        sums = [jnp.zeros((tile_rows, tile_cols), jnp.float32)] * slots
        for i in range(members):
            for b in range(scan_block):
                hour = hours[plane * plane_scans + i * scan_block + b] - base_hour
                depth = jnp.exp(gather[d, i, b] * slope_db - offset_zr)
                for k in range(slots):
                    sums[k] = sums[k] + jnp.where(hour == k, depth, 0.0)
        if t < planes - 1:
            for k in range(slots):
                part[d, k] = sums[k]
            for k in range(slots):

                @pl.when(k < span)
                def _():
                    z_copy(d, k).start()

        else:
            for k in range(slots):
                zrecv[plane, k] = sums[k]

    for p in range(planes):

        @pl.when(p != plane)
        def _():
            for k in range(hour_span(p)):
                pltpu.make_async_remote_copy(
                    src_ref=zrecv.at[p, k],
                    dst_ref=zrecv.at[p, k],
                    send_sem=z_send.at[p, k],
                    recv_sem=z_recv.at[p, k],
                    device_id=(p * CORES + core, col),
                    device_id_type=MESH,
                ).wait_recv()

    for h in range(hour_count):
        total = None
        for p in range(planes):
            if first_hour(p) <= h < first_hour(p) + hour_span(p):
                term = zrecv[p, h - first_hour(p)]
                total = term if total is None else total + term
        hourly_ref[h] = total

    for k in range(1, members):
        id_copy(k).wait_send()
    for k in range(1, planes):
        idz_copy(k).wait_send()
    for d in order:
        for k in range(1, members):
            in_copy(d, k).wait_send()
    for d in order[:-1]:
        for k in range(slots):

            @pl.when(k < span)
            def _():
                z_copy(d, k).wait_send()

    def b_wait(k, carry):
        other = (me + k) % devices
        arrival = pltpu.make_async_remote_copy(
            src_ref=psend,
            dst_ref=precv.at[other],
            send_sem=b_send.at[other],
            recv_sem=b_recv.at[other],
            device_id=(other // col_devices, other % col_devices),
            device_id_type=MESH,
        )
        arrival.wait_recv()
        arrival.wait_send()
        return carry

    lax.fori_loop(1, devices, b_wait, 0, unroll=True)
    hour_rows = lax.broadcasted_iota(jnp.int32, (hour_count, basins), 0)
    total = jnp.zeros((hour_count, basins), jnp.float32)
    for o in range(devices):
        for b in range(scan_block):
            hour = hours[o * scan_block + b]
            total = total + jnp.where(hour_rows == hour, precv[o, b : b + 1, :], 0.0)
    mean = total / count
    mean = pltpu.roll(mean, (basins - me * owned) % basins, 1)
    basin_ref[...] = mean[:, :owned]


def write_out(hourly_ref, basin_ref, hourly_out, basin_out, sem):
    pairs = ((hourly_ref, hourly_out), (basin_ref, basin_out))
    copies = [pltpu.make_async_copy(s, d, sem.at[n]) for n, (s, d) in enumerate(pairs)]
    for copy in copies:
        copy.start()
    for copy in copies:
        copy.wait()


def body(reflectivity, scan_hour, basin_ids):
    row_devices = lax.axis_size("row")
    col_devices = lax.axis_size("col")
    scan_block, grid_height, grid_width = reflectivity.shape
    tile_rows = grid_height // row_devices
    tile_cols = grid_width // col_devices
    scan_count = scan_hour.shape[0]
    hour_count = (scan_count + 10) // HOUR_SCANS + 1
    devices = row_devices * col_devices
    owned = grid_height * grid_width // (SEG * BASIN_ROWS) // devices
    planes = row_devices // CORES
    members = CORES * col_devices
    plane_scans = members * scan_block
    slots = max(
        hour_count
        - (scan_count - plane_scans * (p + 1)) // HOUR_SCANS
        - (p * plane_scans) // HOUR_SCANS
        for p in range(planes)
    )
    dims = (row_devices, col_devices, hour_count, slots, tile_rows, tile_cols, owned)
    dma = pltpu.SemaphoreType.DMA
    f32 = jnp.float32
    anywhere = pl.BlockSpec(memory_space=pltpu.HBM)
    inside = pl.BlockSpec(memory_space=pltpu.VMEM)
    hourly, basin = pl.pallas_call(
        functools.partial(kernel, dims),
        out_shape=(
            jax.ShapeDtypeStruct((hour_count, tile_rows, tile_cols), f32),
            jax.ShapeDtypeStruct((hour_count, owned), f32),
        ),
        in_specs=[anywhere] * 3,
        out_specs=(inside, inside),
        scratch_shapes=[
            pltpu.VMEM(reflectivity.shape, f32),
            pltpu.SMEM(scan_hour.shape, jnp.int32),
            pltpu.VMEM(basin_ids.shape[::-1], jnp.int32),
            pltpu.VMEM((planes, members, scan_block, tile_rows, tile_cols), f32),
            pltpu.VMEM((planes, slots, tile_rows, tile_cols), f32),
            pltpu.VMEM((planes, slots, tile_rows, tile_cols), f32),
            pltpu.VMEM((members,) + basin_ids.shape[::-1], jnp.int32),
            pltpu.VMEM((planes, members) + basin_ids.shape[::-1], jnp.int32),
            pltpu.VMEM((scan_block, devices * owned), f32),
            pltpu.VMEM((devices, scan_block, devices * owned), f32),
            pltpu.SemaphoreType.REGULAR((2, max(1, planes - 2))),
            dma((4,)),
            dma((planes,)),
            dma((planes, members)),
            dma((planes, members)),
            dma((planes, slots)),
            dma((planes, slots)),
            dma((members,)),
            dma((members,)),
            dma((planes,)),
            dma((planes,)),
            dma((devices,)),
            dma((devices,)),
        ],
        compiler_params=pltpu.CompilerParams(
            collective_id=0, has_side_effects=True, vmem_limit_bytes=40 * 2**20
        ),
    )(*(pltpu.with_memory_space_constraint(v, pltpu.HBM) for v in (reflectivity, scan_hour, basin_ids.T)))
    hourly, basin = pl.pallas_call(
        write_out,
        out_shape=(
            jax.ShapeDtypeStruct(hourly.shape, f32),
            jax.ShapeDtypeStruct(basin.shape, f32),
        ),
        in_specs=[inside] * 2,
        out_specs=(anywhere, anywhere),
        scratch_shapes=[dma((2,))],
        compiler_params=pltpu.CompilerParams(vmem_limit_bytes=8 * 2**20),
    )(hourly, basin)
    return hourly, basin.T


def solution(mesh):
    placed = (P(("row", "col"), None, None), P(), P("row", "col"))
    return jax.shard_map(
        body,
        mesh=mesh,
        in_specs=placed,
        out_specs=(P(None, "row", "col"), P(("row", "col"), None)),
        check_vma=False,
    )
```
